32 devices in a mesh: inter: 2 (over y), intra: 16 (over z, x, core).
Axes of the slice: x: 2, y: 2, z: 4, core: 2. Of those that a mesh axis runs over, the one named last changes fastest.
Arguments:
- activations: bfloat16 [65536, 4096], P(('inter', 'intra')), may hold values from -6 to 6
- key_cotangent: bfloat16 [65536, 512], P(('inter', 'intra')), may hold values from -0.046875 to 0.046875
- value_cotangent: bfloat16 [65536, 512], P(('inter', 'intra')), may hold values from -0.046875 to 0.046875
Outputs:
- grad_key: float32 [4096, 512], P('intra')
- grad_value: float32 [4096, 512], P('intra')
The draws below stay inside these ranges and needn't reach their ends.
All inputs are finite; a program needn't handle non-finite values.
Results may differ from the reference program's by a relative error of at most 0.0029.
Values sent between devices are 32-bit elements; how exact they have to be, the bound alone decides.
A program may use at most 128 MiB of HBM per device.

```python
import jax
import jax.numpy as jnp
from jax import lax

D = 4096
TOK_DEV = 2048
KV = 512
TOKENS = 65536
N_INTER = 2
N_INTRA = 16


def levels(key, dims, split, low, largest):
    level, own = 1.0, jax.random.fold_in(key, 6)
    for dim, blocks in split:
        heights = jnp.exp(jax.random.uniform(jax.random.fold_in(own, dim), (blocks,), jnp.float32, low / len(split), largest / len(split)))
        level = level * jnp.repeat(heights, dims[dim] // blocks).reshape([-1 if axis == dim else 1 for axis in range(len(dims))])
    return level


def centred(stream_key, shape, spread, limit, cuts=(), kind=jnp.bfloat16):
    values = spread * jax.random.normal(stream_key, shape, jnp.float32)
    if cuts:
        values = values * levels(stream_key, shape, cuts, -0.22, 0.18)
    return jnp.clip(values, -limit, limit).astype(kind)


def setup_inputs(seed: int = 0) -> dict:
    arg_keys = jax.random.split(jax.random.key(seed), 4)
    activations = centred(arg_keys[0], (TOKENS, D), 1.0, 6.0, ((0, 32),))
    key_cotangent = centred(arg_keys[1], (TOKENS, KV), 0.003, 0.046875, ((0, 32),))
    value_cotangent = centred(arg_keys[2], (TOKENS, KV), 0.003, 0.046875, ((0, 32),))
    return dict(activations=activations, key_cotangent=key_cotangent, value_cotangent=value_cotangent)


def accumulate(total, inputs):
    rows, cotangent = inputs
    device_term = jnp.dot(rows.T, cotangent, preferred_element_type=jnp.float32)
    rounded = lax.optimization_barrier(device_term.astype(jnp.bfloat16))
    return total + rounded.astype(jnp.float32), None


def reference(activations, key_cotangent, value_cotangent):
    devices = N_INTER * N_INTRA
    stacked_rows = activations.reshape(devices, TOK_DEV, D)
    cotangent = jnp.concatenate((key_cotangent, value_cotangent), axis=1).reshape(devices, TOK_DEV, 2 * KV)
    total = lax.scan(accumulate, jnp.zeros((D, 2 * KV), jnp.float32), (stacked_rows, cotangent))[0]
    return total[:, :KV], total[:, KV:]
```

```python
import functools
import heapq

import jax
import jax.numpy as jnp
from jax import lax
from jax.experimental import pallas as pl
from jax.experimental.pallas import tpu as pltpu
from jax.sharding import PartitionSpec as P

MESH = pl.DeviceIdType.MESH


class Message:
    def __init__(self, part, stage, axis, block, target, width, split):
        self.part, self.stage, self.axis = part, stage, axis
        self.block, self.target, self.width, self.split = block, target, width, split
        self.slot = None


def plan_messages(groups, columns):
    bits = tuple(("z", b) for b in range(groups.bit_length() - 1))
    x, y, gather, both = ("x", 0), ("y", 0), ("gather", 0), ("both", 0)
    parts = (
        (0, columns // 2, (x, y) + bits + (gather,)),
        (columns // 2, columns // 4, (y, x) + bits + (gather,)),
        (3 * columns // 4, columns // 4, bits + (x, both)),
    )
    messages = []
    for part, (_, width, stages) in enumerate(parts):
        live, split = list(range(2 * groups)), False
        for stage, axis in enumerate(stages):
            kind, bit = axis
            if kind == "y":
                width, split = width // 2, True
                messages += [Message(part, stage, axis, k, k, width, split) for k in live]
            elif kind in ("gather", "both"):
                messages.append(Message(part, stage, axis, 0, 0, width, split))
            else:
                step = 1 if kind == "x" else 2 << bit
                sent = [k for k in live if k & step]
                messages += [Message(part, stage, axis, k, k - step, width, split) for k in sent]
                live = [k for k in live if not k & step]
    counts = {}
    for message in messages:
        message.slot = counts.get(message.width, 0)
        counts[message.width] = message.slot + 1
    return parts, messages, counts


def block_order(groups):
    return sorted(range(2 * groups), key=lambda k: (-((k >> 1) & 1) - (k & 1), -((k >> 1) & 1), -k))


def schedule(messages, order, rows):
    sends = {(m.part, m.block): [] for m in messages}
    for m in messages:
        sends[m.part, m.block].append(m)
    ready_at = {k: 4.0 + 2.7 * (i + 1) for i, k in enumerate(order)}
    link_free, heap, handled, done = {}, [], [], set()

    def needed(message):
        return [
            o
            for o in messages
            if o.part == message.part and o.target == message.block and o.stage < message.stage
        ]

    def issue(message, now):
        link = "y" if message.axis[0] in ("y", "gather", "both") else message.axis[0]
        start = max(now, link_free.get(link, 0.0))
        link_free[link] = start + message.width * rows * 4 / 46.6e3
        heapq.heappush(heap, (link_free[link] + 2.0, messages.index(message), message))

    initial = {k: [m for m in messages if m.block == k and not needed(m)] for k in order}
    waiting = [m for m in messages if needed(m)]
    for k in order:
        for m in initial[k]:
            issue(m, ready_at[k])
    loop_end = max(ready_at.values()) + 2.0
    now = loop_end
    actions = []
    while heap:
        at, _, message = heapq.heappop(heap)
        now = max(now, at)
        done.add(message)
        follow = [m for m in waiting if all(o in done for o in needed(m))]
        waiting = [m for m in waiting if m not in follow]
        for m in follow:
            issue(m, now)
        actions.append((message, follow))
    return initial, actions


def kernel(
    mesh_shape, plan, order, steps,
    a_hbm, key_hbm, value_hbm, key_out, value_out,
    a_ref, cot_ref, pair_ref, mate_ref, wide_ref, half_ref, quarter_ref,
    a_sem, cot_sem, mate_send, mate_recv, send_sem, recv_sem,
):
    parts, messages = plan
    initial, actions = steps
    groups = mesh_shape["intra"] // 4
    blocks = 2 * groups
    rows = key_out.shape[0]
    tall = 2 * rows
    half = key_hbm.shape[1]
    landing = {ref.shape[2]: ref for ref in (wide_ref, half_ref, quarter_ref)}

    y = lax.axis_index("inter")
    me = lax.axis_index("intra")
    core = me % 2
    x = (me // 2) % 2
    group = me // 4

    def flipped(k):
        place = (x + k % 2) % 2
        for b in range(groups.bit_length() - 1):
            place = place + 2 * (1 << b) * ((group // (1 << b) + k // (2 << b)) % 2)
        return place

    def partner(axis):
        kind, bit = axis
        if kind == "core":
            return {"intra": me + 1 - 2 * core}
        if kind == "x":
            return {"intra": me + 2 * (1 - 2 * x)}
        if kind == "z":
            return {"intra": me + (4 << bit) * (1 - 2 * ((group // (1 << bit)) % 2))}
        return {"inter": 1 - y}

    cot_copies = [
        pltpu.make_async_copy(key_hbm, cot_ref.at[:, pl.ds(0, half)], cot_sem.at[0]),
        pltpu.make_async_copy(value_hbm, cot_ref.at[:, pl.ds(half, half)], cot_sem.at[1]),
    ]
    for copy in cot_copies:
        copy.start()

    def a_copy(i, k):
        columns = pl.ds(pl.multiple_of(flipped(k) * tall, tall), tall)
        return pltpu.make_async_copy(a_hbm.at[:, columns], a_ref.at[i], a_sem.at[i])

    for i, k in enumerate(order):
        a_copy(i, k).start()

    barrier = pltpu.get_barrier_semaphore()
    neighbours = [("core", 0), ("x", 0), ("y", 0)]
    neighbours += [("z", b) for b in range(groups.bit_length() - 1)]
    for axis in neighbours:
        pl.semaphore_signal(barrier, inc=1, device_id=partner(axis), device_id_type=MESH)
    pl.semaphore_wait(barrier, len(neighbours))

    def mate_copy(i):
        return pltpu.make_async_remote_copy(
            src_ref=pair_ref.at[i, 1 - core],
            dst_ref=mate_ref.at[i],
            send_sem=mate_send.at[i],
            recv_sem=mate_recv.at[i],
            device_id=partner(("core", 0)),
            device_id_type=MESH,
        )

    place = {k: i for i, k in enumerate(order)}

    def columns_of(message, mine):
        base, width, _ = parts[message.part]
        if not message.split:
            return pl.ds(base, width)
        side = y if mine else 1 - y
        return pl.ds(pl.multiple_of(base + side * message.width, 128), message.width)

    def remote(message):
        number = messages.index(message)
        mine = message.axis[0] != "y"
        return pltpu.make_async_remote_copy(
            src_ref=pair_ref.at[place[message.block], core, :, columns_of(message, mine)],
            dst_ref=landing[message.width].at[message.slot],
            send_sem=send_sem.at[number],
            recv_sem=recv_sem.at[number],
            device_id=partner(message.axis),
            device_id_type=MESH,
        )

    def finish(i):
        mate_copy(i).wait_recv()
        pair_ref[i, core] += mate_ref[i]
        for j, k in enumerate(order):
            @pl.when(i == j)
            def _():
                for message in initial[k]:
                    remote(message).start()

    for copy in cot_copies:
        copy.wait()

    def body(i, carry):
        pltpu.make_async_copy(
            a_hbm.at[:, pl.ds(0, tall)], a_ref.at[i], a_sem.at[i]
        ).wait()
        product = lax.dot_general(
            a_ref[i], cot_ref[...], (((0,), (0,)), ((), ())),
            preferred_element_type=jnp.float32,
        )
        rounded = product.astype(jnp.bfloat16).astype(jnp.float32)
        pair_ref[i] = rounded.reshape(2, rows, 2 * half)
        mate_copy(i).start()

        @pl.when(i > 0)
        def _():
            finish(i - 1)

        return carry

    lax.fori_loop(0, blocks, body, 0)
    finish(blocks - 1)

    def result(base, width):
        if base < half:
            return key_out, pl.ds(base, width)
        return value_out, pl.ds(base - half, width)

    first = place[0]
    for message, follow in actions:
        remote(message).wait_recv()
        base, width, _ = parts[message.part]
        arrived = landing[message.width].at[message.slot]
        kind = message.axis[0]
        if kind == "both":
            out, columns = result(base, width)
            out[:, columns] = pair_ref[first, core, :, pl.ds(base, width)] + arrived[...]
        elif kind == "gather":
            out = result(base, width)[0]
            start = base if base < half else base - half
            columns = pl.ds(pl.multiple_of(start + (1 - y) * message.width, 128), message.width)
            out[:, columns] = arrived[...]
        else:
            i = place[message.target]
            columns = columns_of(message, True)
            pair_ref[i, core, :, columns] += arrived[...]
        for later in follow:
            remote(later).start()
            if later.axis[0] == "gather":
                base, width, _ = parts[later.part]
                out = result(base, width)[0]
                start = base if base < half else base - half
                columns = pl.ds(pl.multiple_of(start + y * later.width, 128), later.width)
                out[:, columns] = pair_ref[first, core, :, columns_of(later, True)]

    for i in range(blocks):
        mate_copy(i).wait_send()
    for message in messages:
        remote(message).wait_send()


def local(mesh_shape, activations, key_cotangent, value_cotangent):
    tokens, width = activations.shape
    half = key_cotangent.shape[1]
    rows = width // mesh_shape["intra"]
    groups = mesh_shape["intra"] // 4
    blocks = 2 * groups
    parts, messages, counts = plan_messages(groups, 2 * half)
    order = block_order(groups)
    steps = schedule(messages, order, rows)
    f32 = jnp.float32
    landing = [pltpu.VMEM((counts[w], rows, w), f32) for w in sorted(counts, reverse=True)]
    shape = jax.ShapeDtypeStruct((rows, half), f32)
    return pl.pallas_call(
        functools.partial(kernel, mesh_shape, (parts, messages), order, steps),
        out_shape=(shape, shape),
        in_specs=[pl.BlockSpec(memory_space=pl.ANY)] * 3,
        out_specs=(pl.BlockSpec(memory_space=pltpu.VMEM),) * 2,
        scratch_shapes=[
            pltpu.VMEM((blocks, tokens, 2 * rows), activations.dtype),
            pltpu.VMEM((tokens, 2 * half), key_cotangent.dtype),
            pltpu.VMEM((blocks, 2, rows, 2 * half), f32),
            pltpu.VMEM((blocks, rows, 2 * half), f32),
            *landing,
            pltpu.SemaphoreType.DMA((blocks,)),
            pltpu.SemaphoreType.DMA((2,)),
            pltpu.SemaphoreType.DMA((blocks,)),
            pltpu.SemaphoreType.DMA((blocks,)),
            pltpu.SemaphoreType.DMA((len(messages),)),
            pltpu.SemaphoreType.DMA((len(messages),)),
        ],
        compiler_params=pltpu.CompilerParams(
            collective_id=0, has_side_effects=True, vmem_limit_bytes=67043328
        ),
    )(activations, key_cotangent, value_cotangent)


def solution(mesh):
    mesh_shape = dict(mesh.shape)
    return jax.shard_map(
        functools.partial(local, mesh_shape),
        mesh=mesh,
        in_specs=(
            P(("inter", "intra"), None),
            P(("inter", "intra"), None),
            P(("inter", "intra"), None),
        ),
        out_specs=(P("intra", None), P("intra", None)),
        check_vma=False,
    )
```

```python
import functools
import heapq

import jax
import jax.numpy as jnp
from jax import lax
from jax.experimental import pallas as pl
from jax.experimental.pallas import tpu as pltpu
from jax.sharding import PartitionSpec as P

MESH = pl.DeviceIdType.MESH


class Message:
    def __init__(self, part, stage, axis, block, target, width, split):
        self.part, self.stage, self.axis = part, stage, axis
        self.block, self.target, self.width, self.split = block, target, width, split
        self.slot = None


def plan_messages(groups, columns):
    bits = tuple(("z", b) for b in range(groups.bit_length() - 1))
    x, y, gather, both = ("x", 0), ("y", 0), ("gather", 0), ("both", 0)
    parts = (
        (0, columns // 2, (x, y) + bits + (gather,)),
        (columns // 2, columns // 4, (y, x) + bits + (gather,)),
        (3 * columns // 4, columns // 4, bits + (x, both)),
    )
    messages = []
    for part, (_, width, stages) in enumerate(parts):
        live, split = list(range(2 * groups)), False
        for stage, axis in enumerate(stages):
            kind, bit = axis
            if kind == "y":
                width, split = width // 2, True
                messages += [Message(part, stage, axis, k, k, width, split) for k in live]
            elif kind in ("gather", "both"):
                messages.append(Message(part, stage, axis, 0, 0, width, split))
            else:
                step = 1 if kind == "x" else 2 << bit
                sent = [k for k in live if k & step]
                messages += [Message(part, stage, axis, k, k - step, width, split) for k in sent]
                live = [k for k in live if not k & step]
    counts = {}
    for message in messages:
        message.slot = counts.get(message.width, 0)
        counts[message.width] = message.slot + 1
    return parts, messages, counts


def block_order(groups):
    return sorted(range(2 * groups), key=lambda k: (-((k >> 1) & 1) - (k & 1), -((k >> 1) & 1), -k))


def schedule(messages, order, rows):
    ready_at = {
        (k, h): 4.5 + 1.7 * (2 * i + h + 1) for i, k in enumerate(order) for h in range(2)
    }
    latency, depth = 2.0, {"x": 3, "z": len(order)}

    def needed(message):
        return [
            o
            for o in messages
            if o.part == message.part and o.target == message.block and o.stage < message.stage
        ]

    def length(message):
        far = 2 if message.axis[0] == "z" and message.axis[1] else 1
        return far * message.width * rows * 4 / 46.6e3

    @functools.cache
    def tail(message):
        after = [
            latency + length(o) + tail(o)
            for o in messages
            if o.part == message.part and o.block == message.target and o.stage > message.stage
        ]
        return max(after, default=0.0)

    def link(message):
        return "y" if message.axis[0] in ("y", "gather", "both") else message.axis[0]

    initial, actions, done, heap = {}, [], set(), []
    link_free, flying, queued = {}, {}, {"x": [], "z": []}

    def issue(ready, now):
        started = []
        for message in ready:
            if link(message) in queued:
                queued[link(message)].append(message)
            else:
                started.append(message)
        for name, queue in queued.items():
            queue.sort(key=tail, reverse=True)
            while queue and flying.get(name, 0) < depth[name]:
                started.append(queue.pop(0))
                flying[name] = flying.get(name, 0) + 1
        for message in started:
            begin = max(now, link_free.get(link(message), 0.0))
            link_free[link(message)] = begin + length(message)
            arrival = begin + length(message) + latency
            heapq.heappush(heap, (arrival, messages.index(message), message))
        return started

    for k, h in ready_at:
        mine = [m for m in messages if m.block == k and (m.part > 0) == h and not needed(m)]
        initial[k, h] = issue(mine, ready_at[k, h])
    waiting = [m for m in messages if needed(m)]
    now = max(ready_at.values())
    depth["z"] = 2
    while heap:
        at, _, message = heapq.heappop(heap)
        now = max(now, at)
        done.add(message)
        if link(message) in queued:
            flying[link(message)] -= 1
        ready = [m for m in waiting if all(o in done for o in needed(m))]
        waiting = [m for m in waiting if m not in ready]
        actions.append((message, issue(ready, now)))
    return initial, actions


def kernel(
    mesh_shape, plan, order, steps,
    a_hbm, key_hbm, value_hbm, key_out, value_out,
    a_ref, cot_ref, pair_ref, mate_ref, wide_ref, half_ref, quarter_ref,
    a_sem, cot_sem, mate_send, mate_recv, send_sem, recv_sem,
):
    parts, messages = plan
    initial, actions = steps
    groups = mesh_shape["intra"] // 4
    blocks = 2 * groups
    rows = key_out.shape[0]
    tall = 2 * rows
    half = key_hbm.shape[1]
    landing = {ref.shape[2]: ref for ref in (wide_ref, half_ref, quarter_ref)}

    y = lax.axis_index("inter")
    me = lax.axis_index("intra")
    core = me % 2
    x = (me // 2) % 2
    group = me // 4

    def flipped(k):
        place = (x + k % 2) % 2
        for b in range(groups.bit_length() - 1):
            place = place + 2 * (1 << b) * ((group // (1 << b) + k // (2 << b)) % 2)
        return place

    def partner(axis):
        kind, bit = axis
        if kind == "core":
            return {"intra": me + 1 - 2 * core}
        if kind == "x":
            return {"intra": me + 2 * (1 - 2 * x)}
        if kind == "z":
            return {"intra": me + (4 << bit) * (1 - 2 * ((group // (1 << bit)) % 2))}
        return {"inter": 1 - y}

    cot_copies = [
        pltpu.make_async_copy(key_hbm, cot_ref.at[:, pl.ds(0, half)], cot_sem.at[0]),
        pltpu.make_async_copy(value_hbm, cot_ref.at[:, pl.ds(half, half)], cot_sem.at[1]),
    ]
    cot_copies[0].start()

    def a_copy(i, k):
        columns = pl.ds(pl.multiple_of(flipped(k) * tall, tall), tall)
        return pltpu.make_async_copy(a_hbm.at[:, columns], a_ref.at[i], a_sem.at[i])

    a_copy(0, order[0]).start()

    barrier = pltpu.get_barrier_semaphore()
    neighbours = [("core", 0), ("x", 0), ("y", 0)]
    neighbours += [("z", b) for b in range(groups.bit_length() - 1)]
    for axis in neighbours:
        pl.semaphore_signal(barrier, inc=1, device_id=partner(axis), device_id_type=MESH)
    pl.semaphore_wait(barrier, len(neighbours))

    def side(h):
        return pl.ds(h * half, half)

    def mate_copy(i, h):
        return pltpu.make_async_remote_copy(
            src_ref=pair_ref.at[i, 1 - core, :, side(h)],
            dst_ref=mate_ref.at[i, h],
            send_sem=mate_send.at[i, h],
            recv_sem=mate_recv.at[i, h],
            device_id=partner(("core", 0)),
            device_id_type=MESH,
        )

    place = {k: i for i, k in enumerate(order)}

    def columns_of(message, mine):
        base, width, _ = parts[message.part]
        if not message.split:
            return pl.ds(base, width)
        side = y if mine else 1 - y
        return pl.ds(pl.multiple_of(base + side * message.width, 128), message.width)

    def remote(message):
        number = messages.index(message)
        mine = message.axis[0] != "y"
        return pltpu.make_async_remote_copy(
            src_ref=pair_ref.at[place[message.block], core, :, columns_of(message, mine)],
            dst_ref=landing[message.width].at[message.slot],
            send_sem=send_sem.at[number],
            recv_sem=recv_sem.at[number],
            device_id=partner(message.axis),
            device_id_type=MESH,
        )

    def finish(i, h):
        mate_copy(i, h).wait_recv()
        pair_ref[i, core, :, side(h)] += mate_ref[i, h]
        for j, k in enumerate(order):
            if initial[k, h]:
                @pl.when(i == j)
                def _():
                    for message in initial[k, h]:
                        remote(message).start()

    def multiply(i, h):
        product = lax.dot_general(
            a_ref[i], cot_ref[:, side(h)], (((0,), (0,)), ((), ())),
            preferred_element_type=jnp.float32,
        )
        rounded = product.astype(jnp.bfloat16).astype(jnp.float32)
        pair_ref[i, :, :, side(h)] = rounded.reshape(2, rows, half)
        mate_copy(i, h).start()

    cot_copies[0].wait()

    def body(i, carry):
        pltpu.make_async_copy(
            a_hbm.at[:, pl.ds(0, tall)], a_ref.at[i], a_sem.at[i]
        ).wait()

        @pl.when(i == 0)
        def _():
            cot_copies[1].start()

        for j, k in enumerate(order[1:]):
            @pl.when(i == j)
            def _():
                a_copy(j + 1, k).start()

        multiply(i, 0)

        @pl.when(i > 0)
        def _():
            finish(i - 1, 1)

        @pl.when(i == 0)
        def _():
            cot_copies[1].wait()

        multiply(i, 1)
        finish(i, 0)
        return carry

    lax.fori_loop(0, blocks, body, 0)
    finish(blocks - 1, 1)

    def result(base, width):
        if base < half:
            return key_out, pl.ds(base, width)
        return value_out, pl.ds(base - half, width)

    first = place[0]
    for message, follow in actions:
        remote(message).wait_recv()
        base, width, _ = parts[message.part]
        arrived = landing[message.width].at[message.slot]
        kind = message.axis[0]
        if kind == "both":
            out, columns = result(base, width)
            out[:, columns] = pair_ref[first, core, :, pl.ds(base, width)] + arrived[...]
        elif kind == "gather":
            out = result(base, width)[0]
            start = base if base < half else base - half
            columns = pl.ds(pl.multiple_of(start + (1 - y) * message.width, 128), message.width)
            out[:, columns] = arrived[...]
        else:
            i = place[message.target]
            columns = columns_of(message, True)
            pair_ref[i, core, :, columns] += arrived[...]
        for later in follow:
            remote(later).start()
            if later.axis[0] == "gather":
                base, width, _ = parts[later.part]
                out = result(base, width)[0]
                start = base if base < half else base - half
                columns = pl.ds(pl.multiple_of(start + y * later.width, 128), later.width)
                out[:, columns] = pair_ref[first, core, :, columns_of(later, True)]

    for i in range(blocks):
        for h in range(2):
            mate_copy(i, h).wait_send()
    for message in messages:
        remote(message).wait_send()


def local(mesh_shape, activations, key_cotangent, value_cotangent):
    tokens, width = activations.shape
    half = key_cotangent.shape[1]
    rows = width // mesh_shape["intra"]
    groups = mesh_shape["intra"] // 4
    blocks = 2 * groups
    parts, messages, counts = plan_messages(groups, 2 * half)
    order = block_order(groups)
    steps = schedule(messages, order, rows)
    f32 = jnp.float32
    landing = [pltpu.VMEM((counts[w], rows, w), f32) for w in sorted(counts, reverse=True)]
    shape = jax.ShapeDtypeStruct((rows, half), f32)
    return pl.pallas_call(
        functools.partial(kernel, mesh_shape, (parts, messages), order, steps),
        out_shape=(shape, shape),
        in_specs=[pl.BlockSpec(memory_space=pl.ANY)] * 3,
        out_specs=(pl.BlockSpec(memory_space=pltpu.VMEM),) * 2,
        scratch_shapes=[
            pltpu.VMEM((blocks, tokens, 2 * rows), activations.dtype),
            pltpu.VMEM((tokens, 2 * half), key_cotangent.dtype),
            pltpu.VMEM((blocks, 2, rows, 2 * half), f32),
            pltpu.VMEM((blocks, 2, rows, half), f32),
            *landing,
            pltpu.SemaphoreType.DMA((blocks,)),
            pltpu.SemaphoreType.DMA((2,)),
            pltpu.SemaphoreType.DMA((blocks, 2)),
            pltpu.SemaphoreType.DMA((blocks, 2)),
            pltpu.SemaphoreType.DMA((len(messages),)),
            pltpu.SemaphoreType.DMA((len(messages),)),
        ],
        compiler_params=pltpu.CompilerParams(
            collective_id=0, has_side_effects=True, vmem_limit_bytes=67043328
        ),
    )(activations, key_cotangent, value_cotangent)


def solution(mesh):
    mesh_shape = dict(mesh.shape)
    return jax.shard_map(
        functools.partial(local, mesh_shape),
        mesh=mesh,
        in_specs=(
            P(("inter", "intra"), None),
            P(("inter", "intra"), None),
            P(("inter", "intra"), None),
        ),
        out_specs=(P("intra", None), P("intra", None)),
        check_vma=False,
    )
```
